32 devices in a mesh: dp: 8 (over z, core), mp: 4 (over y, x).
Axes of the slice: x: 2, y: 2, z: 4, core: 2. Of those that a mesh axis runs over, the one named last changes fastest.
Arguments:
- features: bfloat16 [8192, 8192], P('dp', 'mp'), may hold values from -6 to 6
- v_weight: bfloat16 [3, 8192, 1024], P(None, 'mp', 'dp'), may hold values from -0.0625 to 0.0625
- u_weight: bfloat16 [3, 1024, 8192], P(None, 'dp', 'mp'), may hold values from -0.1875 to 0.1875
- cross_bias: float32 [3, 8192], P(None, 'mp'), may hold values from -3 to 3
Outputs:
- crossed: bfloat16 [8192, 8192], P('dp', 'mp')
The draws below stay inside these ranges and needn't reach their ends.
All inputs are finite; a program needn't handle non-finite values.
Results may differ from the reference program's by a relative error of at most 0.009.
Values may be sent and summed in bfloat16 or wider, within the bound.
A program may use at most 128 MiB of HBM per device.

```python
import jax
import jax.numpy as jnp

D = 8192
R = 1024
LAYERS = 3
BATCH = 8192


def block_levels(key, extent, split, low, top_value):
    factor_of = 1.0
    for axis_at, blocks in split:
        draws = jax.random.uniform(jax.random.fold_in(jax.random.fold_in(key, 6), axis_at), (blocks,), jnp.float32, low / len(split), top_value / len(split))
        factor_of = factor_of * jnp.repeat(jnp.exp(draws), extent[axis_at] // blocks).reshape((-1,) + (1,) * (len(extent) - 1 - axis_at))
    return factor_of


def scatter_about(key, shape, width, reach, shards=(), kind=jnp.bfloat16):
    entries = jax.random.normal(key, shape, jnp.float32) * width
    if len(shards) > 0:
        entries = block_levels(key, shape, shards, -0.22, 0.18) * entries
    return jnp.clip(entries, min=-reach, max=reach).astype(kind)


def setup_inputs(seed: int = 0) -> dict:
    key_of = jax.random.split(jax.random.key(seed), 5)
    features = scatter_about(key_of[0], (BATCH, D), 1.0, 6.0, ((0, 8), (1, 4)))
    v_weight = scatter_about(key_of[1], (LAYERS, D, R), D ** -0.5, 0.0625, ((1, 4), (2, 8)))
    u_weight = scatter_about(key_of[2], (LAYERS, R, D), R ** -0.5, 0.1875, ((1, 8), (2, 4)))
    cross_bias = scatter_about(key_of[3], (LAYERS, D), 0.5, 3.0, ((1, 4),), jnp.float32)
    return {"features": features, "v_weight": v_weight, "u_weight": u_weight, "cross_bias": cross_bias}


def reference(features, v_weight, u_weight, cross_bias):
    carried = features
    for layer_number in range(LAYERS):
        rank_proj = jnp.dot(carried, v_weight[layer_number], preferred_element_type=jnp.float32).astype(jnp.bfloat16)
        cross_term = jnp.dot(rank_proj, u_weight[layer_number], preferred_element_type=jnp.float32) + cross_bias[layer_number]
        carried = (features.astype(jnp.float32) * cross_term + carried.astype(jnp.float32)).astype(jnp.bfloat16)
    return carried
```

```python
import functools

import jax
import jax.numpy as jnp
from jax import lax
from jax.experimental import pallas as pl
from jax.experimental.pallas import tpu as pltpu
from jax.sharding import PartitionSpec as P

MESH = pl.DeviceIdType.MESH
HOPS = (1, -1)


def kernel(nz, n, native, nb, v_ref, u_ref, x_ref, b_ref, out_ref, wv, wu, f_ref, pf, sbuf, rbuf,
           rank, loc, zsend, zrecv, fsend, psend, precv, rs_s, rs_r, ag_s, ag_r, in_s):
    layers, rs, cols = u_ref.shape
    rows = x_ref.shape[0]
    seg = rows // n
    ck = 2 * rs
    tail = 2 * layers - 1
    pieces = tail + nb
    bw = cols // nb

    def at_sem(p):
        return tail + p[0] if isinstance(p, tuple) else p

    def each_piece(body):
        for p in range(tail):
            body(p)
        each_tail(body)

    def each_tail(body):
        @pl.loop(0, nb)
        def _(b):
            body((b,))

    cb = 256 if cols % 256 == 0 else cols
    dp, me = lax.axis_index("dp"), lax.axis_index("mp")
    z, c = dp // 2, dp % 2
    step = jnp.where(2 * z < nz, 1, -1)
    end = (z == 0) | (z == nz - 1)

    def dev(zt, ct, m):
        return {"dp": zt * 2 + ct, "mp": m}

    def copy_to(src, dst, send, recv, device):
        return pltpu.make_async_remote_copy(
            src_ref=src, dst_ref=dst, send_sem=send, recv_sem=recv,
            device_id=device, device_id_type=MESH)

    def order(i):
        near = jnp.minimum(z, nz - 1 - z)
        zigzag = jnp.where(i % 2 == 1, -((i + 1) // 2), i // 2)
        return z + step * jnp.where(i <= 2 * near, zigzag, i - near)

    def valid(d):
        return (z + d >= 0) & (z + d < nz)

    def blk(p, s, cc):
        if isinstance(p, tuple):
            return wu.at[layers - 1, pl.ds(pl.multiple_of((s * 2 + cc) * rs, rs), rs),
                         pl.ds(pl.multiple_of(p[0] * bw, bw), bw)]
        if native and p % 2 == 0:
            return wv.at[p // 2, s, :, pl.ds(pl.multiple_of(cc * rs, rs), rs)]
        w = wu if p % 2 else wv
        return w.at[p // 2, pl.ds(pl.multiple_of((s * 2 + cc) * rs, rs), rs)]

    def local_copy(p):
        if isinstance(p, tuple):
            src = u_ref.at[layers - 1, :, pl.ds(pl.multiple_of(p[0] * bw, bw), bw)]
        else:
            src = (v_ref if p % 2 == 0 else u_ref).at[p // 2]
        return pltpu.make_async_copy(src, blk(p, z, c), loc.at[at_sem(p)])

    def direct(p, k):
        return copy_to(blk(p, z, c), blk(p, z, c), zsend.at[at_sem(p), k], zrecv.at[at_sem(p), z],
                       dev(z + HOPS[k], c, me))

    def arrival(p, s):
        return copy_to(blk(p, s, c), blk(p, s, c), fsend.at[at_sem(p), s], zrecv.at[at_sem(p), s], dev(z, 1 - c, me))

    def relays(s):
        return ((s > z) & (z >= 1)) | ((s < z) & (z <= nz - 2))

    def relay(p, s):
        return copy_to(blk(p, s, c), blk(p, s, c), fsend.at[at_sem(p), s], zrecv.at[at_sem(p), s],
                       dev(jnp.where(s > z, z - 1, z + 1), c, me))

    def push(p, s):
        return copy_to(blk(p, s, c), blk(p, s, c), psend.at[at_sem(p), s], precv.at[at_sem(p), s], dev(z, 1 - c, me))

    def pushed(p, s):
        return copy_to(blk(p, s, 1 - c), blk(p, s, 1 - c), psend.at[at_sem(p), s], precv.at[at_sem(p), s],
                       dev(z, 1 - c, me))

    def held(d):
        return (z >= 1) & (z <= nz - 2)

    def issue_own(p, first):
        for k in range(len(HOPS)):
            hold = held(HOPS[k])

            @pl.when(valid(HOPS[k]) & (jnp.logical_not(hold) if first else hold))
            def _():
                direct(p, k).start()

    def take(p, s):
        @pl.when(s != z)
        def _():
            arrival(p, s).wait_recv()

        @pl.when(relays(s))
        def _():
            relay(p, s).start()

        push(p, s).start()

    def lanes(s):
        return pl.ds(pl.multiple_of(s * ck, ck), ck)

    def seg_rows(m):
        return pl.ds(pl.multiple_of(m * seg, seg), seg)

    def other(k):
        return lax.rem(me + k, n)

    def drain(p):
        for k in range(len(HOPS)):
            @pl.when(valid(HOPS[k]))
            def _():
                direct(p, k).wait_send()

        @pl.loop(0, nz)
        def _(s):
            push(p, s).wait_send()

            @pl.when(relays(s))
            def _():
                relay(p, s).wait_send()

    whole_in = pltpu.make_async_copy(x_ref, f_ref, in_s)
    each_piece(lambda p: local_copy(p).start())
    whole_in.start()
    barrier = pltpu.get_barrier_semaphore()
    for k in range(1, n):
        pl.semaphore_signal(barrier, inc=1, device_id=dev(z, c, other(k)), device_id_type=MESH)
    pl.semaphore_signal(barrier, inc=1, device_id=dev(z, 1 - c, me), device_id_type=MESH)
    for d in HOPS:
        @pl.when(valid(d))
        def _():
            pl.semaphore_signal(barrier, inc=1, device_id=dev(z + d, c, me), device_id_type=MESH)
    pl.semaphore_wait(barrier, n + jnp.minimum(z, 1) + jnp.minimum(nz - 1 - z, 1))

    def first_sends(p):
        local_copy(p).wait()
        issue_own(p, True)
        if p in range(min(2, tail)):
            issue_own(p, False)

    each_piece(first_sends)
    whole_in.wait()

    @pl.when(jnp.logical_not(end))
    def _():
        @pl.loop(0, nz)
        def _(i):
            take(0, order(i))

    if layers > 1:
        issue_own(2, False)
    else:
        each_tail(lambda p: issue_own(p, False))

    for l in range(layers):
        pv, pu = 2 * l, 2 * l + 1
        cur = f_ref if l == 0 else out_ref

        def sum_out(s, k):
            t = other(k)
            return copy_to(sbuf.at[seg_rows(t), lanes(s)], rbuf.at[l, me, :, lanes(s)],
                           rs_s.at[s, k - 1], rs_r.at[s, me], dev(z, c, t))

        def sum_in(s, k):
            q = other(k)
            return copy_to(sbuf.at[seg_rows(q), lanes(s)], rbuf.at[l, q, :, lanes(s)],
                           rs_s.at[s, k - 1], rs_r.at[s, q], dev(z, c, q))

        def rank_out(s, k):
            mine = rank.at[l, seg_rows(me), lanes(s)]
            return copy_to(mine, mine, ag_s.at[s, k - 1], ag_r.at[s, me], dev(z, c, other(k)))

        def rank_in(s, k):
            q = other(k)
            theirs = rank.at[l, seg_rows(q), lanes(s)]
            return copy_to(theirs, theirs, ag_s.at[s, k - 1], ag_r.at[s, q], dev(z, c, q))

        def reduce(s):
            acc = pf[seg_rows(me), lanes(s)]
            for k in range(1, n):
                sum_in(s, k).wait_recv()
                acc = acc + rbuf[l, other(k), :, lanes(s)].astype(jnp.float32)
            rank[l, seg_rows(me), lanes(s)] = acc.astype(jnp.bfloat16)
            for k in range(1, n):
                rank_out(s, k).start()

        last = l == layers - 1
        each_up = each_tail if last else lambda body: body(pu)

        @pl.loop(0, nz)
        def _(i):
            s = order(i)

            @pl.when(end)
            def _():
                take(pv, s)

            @pl.when(jnp.logical_not(end))
            def _():
                each_up(lambda p: take(p, s))

            pushed(pv, s).wait_recv()
            if native:
                part = jnp.dot(cur[...], wv[l, s], preferred_element_type=jnp.float32)
            else:
                part = lax.dot_general(cur[...], wv[l, lanes(s), :], (((1,), (1,)), ((), ())),
                                       preferred_element_type=jnp.float32)
            pf[:, lanes(s)] = part
            sbuf[:, lanes(s)] = part.astype(jnp.bfloat16)
            for k in range(1, n):
                sum_out(s, k).start()

            @pl.when(i > 0)
            def _():
                reduce(order(i - 1))

        if pu + 2 < tail:
            issue_own(pu + 2, False)
        elif not last and layers > 2:
            issue_own(pv + 2, False)

        reduce(order(nz - 1))
        if last:
            for p in range(tail - 1):
                drain(p)

        @pl.loop(0, nz - 1)
        def _(i):
            s = order(i)

            @pl.when(end)
            def _():
                each_up(lambda p: take(p, s))

            if not last:
                @pl.when(jnp.logical_not(end))
                def _():
                    take(pv + 2, s)

        if not last:
            @pl.when(jnp.logical_not(end))
            def _():
                take(pv + 2, order(nz - 1))

            if pv + 4 < tail - 1:
                issue_own(pv + 4, False)
            elif pv + 4 > tail:
                each_tail(lambda p: issue_own(p, False))

        @pl.loop(0, nz)
        def _(i):
            for k in range(1, n):
                rank_in(order(i), k).wait_recv()

        def finish(p):
            @pl.when(end)
            def _():
                take(p, order(nz - 1))

            @pl.loop(0, nz)
            def _(i):
                pushed(p, order(i)).wait_recv()

            width, base = (bw, p[0] * bw) if last else (cols, 0)

            @pl.loop(0, width // cb)
            def _(j):
                at = pl.ds(pl.multiple_of(base + j * cb, cb), cb)
                cross = jnp.dot(rank[l], wu[l, :, at], preferred_element_type=jnp.float32)
                cross = cross + b_ref[l, at][None, :]
                out_ref[:, at] = (f_ref[:, at].astype(jnp.float32) * cross
                                  + cur[:, at].astype(jnp.float32)).astype(jnp.bfloat16)

        each_up(finish)

        @pl.loop(0, nz)
        def _(s):
            for k in range(1, n):
                sum_out(s, k).wait_send()
                rank_out(s, k).wait_send()

    for p in range(max(tail - 1, 0), tail):
        drain(p)
    each_tail(drain)


def solution(mesh):
    n = mesh.shape["mp"]
    nz = mesh.shape["dp"] // 2

    def local(features, v_weight, u_weight, cross_bias):
        layers, rs, cols = u_weight.shape
        rows = features.shape[0]
        r = rs * nz * 2
        nb = 4 if cols % 512 == 0 else 1
        pieces = 2 * layers - 1 + nb
        native = rs % 128 == 0
        v = v_weight if native else jnp.swapaxes(v_weight, 1, 2)
        vm = pl.BlockSpec(memory_space=pltpu.VMEM)
        hbm = pl.BlockSpec(memory_space=pl.ANY)
        dma = pltpu.SemaphoreType.DMA
        return pl.pallas_call(
            functools.partial(kernel, nz, n, native, nb),
            out_shape=pltpu.VMEM((rows, cols), jnp.bfloat16),
            in_specs=[hbm, hbm, hbm, vm],
            out_specs=vm,
            scratch_shapes=[
                pltpu.VMEM((layers, nz, cols, 2 * rs) if native else (layers, r, cols), jnp.bfloat16),
                pltpu.VMEM((layers, r, cols), jnp.bfloat16),
                pltpu.VMEM((rows, cols), jnp.bfloat16),
                pltpu.VMEM((rows, r), jnp.float32),
                pltpu.VMEM((rows, r), jnp.bfloat16),
                pltpu.VMEM((layers, n, rows // n, r), jnp.bfloat16),
                pltpu.VMEM((layers, rows, r), jnp.bfloat16),
                dma((pieces,)), dma((pieces, len(HOPS))), dma((pieces, nz)), dma((pieces, nz)),
                dma((pieces, nz)), dma((pieces, nz)),
                dma((nz, n)), dma((nz, n)), dma((nz, n)), dma((nz, n)),
                dma,
            ],
            compiler_params=pltpu.CompilerParams(
                collective_id=0, has_side_effects=True, vmem_limit_bytes=59*2**20),
            name="cross_layers",
        )(v, u_weight, features, cross_bias)

    return jax.shard_map(
        local,
        mesh=mesh,
        in_specs=(P("dp", "mp"), P(None, "mp", "dp"), P(None, "dp", "mp"), P(None, "mp")),
        out_specs=P("dp", "mp"),
        check_vma=False,
    )
```

```python
import functools

import jax
import jax.numpy as jnp
from jax import lax
from jax.experimental import pallas as pl
from jax.experimental.pallas import tpu as pltpu
from jax.sharding import PartitionSpec as P

MESH = pl.DeviceIdType.MESH
HOPS = (1, -1)


def kernel(nz, n, native, nb, v_ref, u_ref, x_ref, b_ref, out_ref, wv, wu, f_ref, pf, sbuf, rbuf,
           rank, loc, zsend, zrecv, fsend, psend, precv, rs_s, rs_r, ag_s, ag_r, in_s):
    layers, rs, cols = u_ref.shape
    rows = x_ref.shape[0]
    seg = rows // n
    ck = 2 * rs
    tail = 2 * layers - 1
    pieces = tail + nb
    bw = cols // nb

    def at_sem(p):
        return tail + p[0] if isinstance(p, tuple) else p

    def each_piece(body):
        for p in range(tail):
            body(p)
        each_tail(body)

    def each_tail(body):
        @pl.loop(0, nb)
        def _(b):
            body((b,))

    cb = 256 if cols % 256 == 0 else cols
    dp, me = lax.axis_index("dp"), lax.axis_index("mp")
    z, c = dp // 2, dp % 2
    step = jnp.where(2 * z < nz, 1, -1)
    end = (z == 0) | (z == nz - 1)

    def dev(zt, ct, m):
        return {"dp": zt * 2 + ct, "mp": m}

    def copy_to(src, dst, send, recv, device):
        return pltpu.make_async_remote_copy(
            src_ref=src, dst_ref=dst, send_sem=send, recv_sem=recv,
            device_id=device, device_id_type=MESH)

    def order(i):
        near = jnp.minimum(z, nz - 1 - z)
        zigzag = jnp.where(i % 2 == 1, -((i + 1) // 2), i // 2)
        return z + step * jnp.where(i <= 2 * near, zigzag, i - near)

    def valid(d):
        return (z + d >= 0) & (z + d < nz)

    def blk(p, s, cc):
        if isinstance(p, tuple):
            return wu.at[layers - 1, pl.ds(pl.multiple_of((s * 2 + cc) * rs, rs), rs),
                         pl.ds(pl.multiple_of(p[0] * bw, bw), bw)]
        if native and p % 2 == 0:
            return wv.at[p // 2, s, :, pl.ds(pl.multiple_of(cc * rs, rs), rs)]
        w = wu if p % 2 else wv
        return w.at[p // 2, pl.ds(pl.multiple_of((s * 2 + cc) * rs, rs), rs)]

    def local_copy(p):
        if isinstance(p, tuple):
            src = u_ref.at[layers - 1, :, pl.ds(pl.multiple_of(p[0] * bw, bw), bw)]
        else:
            src = (v_ref if p % 2 == 0 else u_ref).at[p // 2]
        return pltpu.make_async_copy(src, blk(p, z, c), loc.at[at_sem(p)])

    def direct(p, k):
        return copy_to(blk(p, z, c), blk(p, z, c), zsend.at[at_sem(p), k], zrecv.at[at_sem(p), z],
                       dev(z + HOPS[k], c, me))

    def arrival(p, s):
        return copy_to(blk(p, s, c), blk(p, s, c), fsend.at[at_sem(p), s], zrecv.at[at_sem(p), s], dev(z, 1 - c, me))

    def relays(s):
        return ((s > z) & (z >= 1)) | ((s < z) & (z <= nz - 2))

    def relay(p, s):
        return copy_to(blk(p, s, c), blk(p, s, c), fsend.at[at_sem(p), s], zrecv.at[at_sem(p), s],
                       dev(jnp.where(s > z, z - 1, z + 1), c, me))

    def push(p, s):
        return copy_to(blk(p, s, c), blk(p, s, c), psend.at[at_sem(p), s], precv.at[at_sem(p), s], dev(z, 1 - c, me))

    def pushed(p, s):
        return copy_to(blk(p, s, 1 - c), blk(p, s, 1 - c), psend.at[at_sem(p), s], precv.at[at_sem(p), s],
                       dev(z, 1 - c, me))

    def held(d):
        return (z >= 1) & (z <= nz - 2)

    def to_end(k):
        return (z + HOPS[k] == 0) | (z + HOPS[k] == nz - 1)

    def issue_own(p, first, k_ok=lambda k: True):
        for k in range(len(HOPS)):
            hold = held(HOPS[k])

            @pl.when(valid(HOPS[k]) & (jnp.logical_not(hold) if first else hold) & (k_ok(k)))
            def _():
                direct(p, k).start()

    def take(p, s):
        @pl.when(s != z)
        def _():
            arrival(p, s).wait_recv()

        @pl.when(relays(s))
        def _():
            relay(p, s).start()

        push(p, s).start()

    def lanes(s):
        return pl.ds(pl.multiple_of(s * ck, ck), ck)

    def seg_rows(m):
        return pl.ds(pl.multiple_of(m * seg, seg), seg)

    def other(k):
        return lax.rem(me + k, n)

    def drain(p, pushes=nz):
        for k in range(len(HOPS)):
            @pl.when(valid(HOPS[k]))
            def _():
                direct(p, k).wait_send()

        @pl.loop(0, pushes)
        def _(i):
            s = order(i)
            push(p, s).wait_send()

            @pl.when(relays(s))
            def _():
                relay(p, s).wait_send()

    whole_in = pltpu.make_async_copy(x_ref, f_ref, in_s)
    barrier = pltpu.get_barrier_semaphore()
    for k in range(1, n):
        pl.semaphore_signal(barrier, inc=1, device_id=dev(z, c, other(k)), device_id_type=MESH)
    pl.semaphore_signal(barrier, inc=1, device_id=dev(z, 1 - c, me), device_id_type=MESH)
    for d in HOPS:
        @pl.when(valid(d))
        def _():
            pl.semaphore_signal(barrier, inc=1, device_id=dev(z + d, c, me), device_id_type=MESH)
    each_piece(lambda p: local_copy(p).start())
    whole_in.start()
    pl.semaphore_wait(barrier, n + jnp.minimum(z, 1) + jnp.minimum(nz - 1 - z, 1))

    def first_sends(p):
        local_copy(p).wait()
        issue_own(p, True)
        if p == 0:
            issue_own(p, False)
        if p == 1:
            issue_own(p, False, to_end)

    each_piece(first_sends)
    whole_in.wait()

    @pl.when(jnp.logical_not(end))
    def _():
        @pl.loop(0, nz)
        def _(i):
            take(0, order(i))

    if tail > 1:
        issue_own(1, False, lambda k: jnp.logical_not(to_end(k)))
    if layers > 1:
        issue_own(2, False)
    else:
        each_tail(lambda p: issue_own(p, False))

    for l in range(layers):
        pv, pu = 2 * l, 2 * l + 1
        cur = f_ref if l == 0 else out_ref

        def sum_out(s, k):
            t = other(k)
            return copy_to(sbuf.at[seg_rows(t), lanes(s)], rbuf.at[l, me, :, lanes(s)],
                           rs_s.at[s, k - 1], rs_r.at[s, me], dev(z, c, t))

        def sum_in(s, k):
            q = other(k)
            return copy_to(sbuf.at[seg_rows(q), lanes(s)], rbuf.at[l, q, :, lanes(s)],
                           rs_s.at[s, k - 1], rs_r.at[s, q], dev(z, c, q))

        def rank_out(s, k):
            mine = rank.at[l, seg_rows(me), lanes(s)]
            return copy_to(mine, mine, ag_s.at[s, k - 1], ag_r.at[s, me], dev(z, c, other(k)))

        def rank_in(s, k):
            q = other(k)
            theirs = rank.at[l, seg_rows(q), lanes(s)]
            return copy_to(theirs, theirs, ag_s.at[s, k - 1], ag_r.at[s, q], dev(z, c, q))

        def reduce(s):
            acc = pf[seg_rows(me), lanes(s)]
            for k in range(1, n):
                sum_in(s, k).wait_recv()
                acc = acc + rbuf[l, other(k), :, lanes(s)].astype(jnp.float32)
            rank[l, seg_rows(me), lanes(s)] = acc.astype(jnp.bfloat16)
            for k in range(1, n):
                rank_out(s, k).start()

        last = l == layers - 1
        each_up = each_tail if last else lambda body: body(pu)

        @pl.loop(0, nz)
        def _(i):
            s = order(i)

            @pl.when(i == nz - 1)
            def _():
                reduce(order(i - 1))

            @pl.when(end)
            def _():
                take(pv, s)

            @pl.when(jnp.logical_not(end))
            def _():
                each_up(lambda p: take(p, s))

            pushed(pv, s).wait_recv()
            if native:
                part = jnp.dot(cur[...], wv[l, s], preferred_element_type=jnp.float32)
            else:
                part = lax.dot_general(cur[...], wv[l, lanes(s), :], (((1,), (1,)), ((), ())),
                                       preferred_element_type=jnp.float32)
            pf[:, lanes(s)] = part
            sbuf[:, lanes(s)] = part.astype(jnp.bfloat16)
            for k in range(1, n):
                sum_out(s, k).start()

            @pl.when((i > 0) & (i < nz - 1))
            def _():
                reduce(order(i - 1))

        if pu + 2 < tail:
            issue_own(pu + 2, False)
        elif not last and layers > 2:
            issue_own(pv + 2, False)

        reduce(order(nz - 1))

        @pl.loop(0, nz - 1)
        def _(i):
            s = order(i)

            @pl.when(end)
            def _():
                each_up(lambda p: take(p, s))

            if not last:
                @pl.when(jnp.logical_not(end))
                def _():
                    take(pv + 2, s)

        if not last:
            @pl.when(jnp.logical_not(end))
            def _():
                take(pv + 2, order(nz - 1))

            if pv + 4 < tail - 1:
                issue_own(pv + 4, False)
            elif pv + 4 > tail:
                each_tail(lambda p: issue_own(p, False))

        if last:
            @pl.when(end)
            def _():
                for p in range(tail):
                    drain(p)
                each_tail(lambda p: drain(p, nz - 1))

        @pl.loop(0, nz)
        def _(i):
            for k in range(1, n):
                rank_in(order(i), k).wait_recv()

        if last:
            @pl.when(end)
            def _():
                take((0,), order(nz - 1))

        def finish(p):
            @pl.when(end)
            def _():
                if last:
                    @pl.when(p[0] < nb - 1)
                    def _():
                        take((p[0] + 1,), order(nz - 1))
                else:
                    take(p, order(nz - 1))

            @pl.loop(0, nz)
            def _(i):
                pushed(p, order(i)).wait_recv()

            width, base = (bw, p[0] * bw) if last else (cols, 0)

            @pl.loop(0, width // cb)
            def _(j):
                at = pl.ds(pl.multiple_of(base + j * cb, cb), cb)
                cross = jnp.dot(rank[l], wu[l, :, at], preferred_element_type=jnp.float32)
                cross = cross + b_ref[l, at][None, :]
                out_ref[:, at] = (f_ref[:, at].astype(jnp.float32) * cross
                                  + cur[:, at].astype(jnp.float32)).astype(jnp.bfloat16)

        @pl.loop(0, nz)
        def _(s):
            for k in range(1, n):
                sum_out(s, k).wait_send()
                rank_out(s, k).wait_send()

        each_up(finish)

    @pl.when(end)
    def _():
        each_tail(lambda p: push(p, order(nz - 1)).wait_send())

    @pl.when(jnp.logical_not(end))
    def _():
        for p in range(tail):
            drain(p)
        each_tail(drain)


def solution(mesh):
    n = mesh.shape["mp"]
    nz = mesh.shape["dp"] // 2

    def local(features, v_weight, u_weight, cross_bias):
        layers, rs, cols = u_weight.shape
        rows = features.shape[0]
        r = rs * nz * 2
        nb = 4 if cols % 512 == 0 else 1
        pieces = 2 * layers - 1 + nb
        native = rs % 128 == 0
        v = v_weight if native else jnp.swapaxes(v_weight, 1, 2)
        vm = pl.BlockSpec(memory_space=pltpu.VMEM)
        hbm = pl.BlockSpec(memory_space=pl.ANY)
        dma = pltpu.SemaphoreType.DMA
        return pl.pallas_call(
            functools.partial(kernel, nz, n, native, nb),
            out_shape=pltpu.VMEM((rows, cols), jnp.bfloat16),
            in_specs=[hbm, hbm, hbm, vm],
            out_specs=vm,
            scratch_shapes=[
                pltpu.VMEM((layers, nz, cols, 2 * rs) if native else (layers, r, cols), jnp.bfloat16),
                pltpu.VMEM((layers, r, cols), jnp.bfloat16),
                pltpu.VMEM((rows, cols), jnp.bfloat16),
                pltpu.VMEM((rows, r), jnp.float32),
                pltpu.VMEM((rows, r), jnp.bfloat16),
                pltpu.VMEM((layers, n, rows // n, r), jnp.bfloat16),
                pltpu.VMEM((layers, rows, r), jnp.bfloat16),
                dma((pieces,)), dma((pieces, len(HOPS))), dma((pieces, nz)), dma((pieces, nz)),
                dma((pieces, nz)), dma((pieces, nz)),
                dma((nz, n)), dma((nz, n)), dma((nz, n)), dma((nz, n)),
                dma,
            ],
            compiler_params=pltpu.CompilerParams(
                collective_id=0, has_side_effects=True, vmem_limit_bytes=59*2**20),
            name="cross_layers",
        )(v, u_weight, features, cross_bias)

    return jax.shard_map(
        local,
        mesh=mesh,
        in_specs=(P("dp", "mp"), P(None, "mp", "dp"), P(None, "dp", "mp"), P(None, "mp")),
        out_specs=P("dp", "mp"),
        check_vma=False,
    )
```

```python
import functools

import jax
import jax.numpy as jnp
from jax import lax
from jax.experimental import pallas as pl
from jax.experimental.pallas import tpu as pltpu
from jax.sharding import PartitionSpec as P

MESH = pl.DeviceIdType.MESH
HOPS = (1, -1)


def kernel(nz, n, native, nb, v_ref, u_ref, x_ref, b_ref, out_ref, wv, wu, f_ref, pf, sbuf, rbuf,
           rank, loc, zsend, zrecv, fsend, psend, vrecv, urecv, rs_s, rs_r, ag_s, ag_r, in_s):
    layers, rs, cols = u_ref.shape
    rows = x_ref.shape[0]
    seg = rows // n
    ck = 2 * rs
    tail = 2 * layers - 1
    pieces = tail + nb
    bw = cols // nb

    def at_sem(p):
        return tail + p[0] if isinstance(p, tuple) else p

    def factor(p):
        return tail if isinstance(p, tuple) else p

    def each_piece(body):
        for p in range(tail):
            body(p)
        each_tail(body)

    def each_tail(body):
        @pl.loop(0, nb)
        def _(b):
            body((b,))

    cb = 256 if cols % 256 == 0 else cols
    dp, me = lax.axis_index("dp"), lax.axis_index("mp")
    z, c = dp // 2, dp % 2
    step = jnp.where(2 * z < nz, 1, -1)
    end = (z == 0) | (z == nz - 1)

    def dev(zt, ct, m):
        return {"dp": zt * 2 + ct, "mp": m}

    def copy_to(src, dst, send, recv, device):
        return pltpu.make_async_remote_copy(
            src_ref=src, dst_ref=dst, send_sem=send, recv_sem=recv,
            device_id=device, device_id_type=MESH)

    def order(i):
        near = jnp.minimum(z, nz - 1 - z)
        zigzag = jnp.where(i % 2 == 1, -((i + 1) // 2), i // 2)
        return z + step * jnp.where(i <= 2 * near, zigzag, i - near)

    def valid(d):
        return (z + d >= 0) & (z + d < nz)

    def blk(p, s, cc):
        if isinstance(p, tuple):
            return wu.at[layers - 1, pl.ds(pl.multiple_of((s * 2 + cc) * rs, rs), rs),
                         pl.ds(pl.multiple_of(p[0] * bw, bw), bw)]
        if native and p % 2 == 0:
            return wv.at[p // 2, s, :, pl.ds(pl.multiple_of(cc * rs, rs), rs)]
        w = wu if p % 2 else wv
        return w.at[p // 2, pl.ds(pl.multiple_of((s * 2 + cc) * rs, rs), rs)]

    def local_copy(p):
        if isinstance(p, tuple):
            src = u_ref.at[layers - 1, :, pl.ds(pl.multiple_of(p[0] * bw, bw), bw)]
        else:
            src = (v_ref if p % 2 == 0 else u_ref).at[p // 2]
        return pltpu.make_async_copy(src, blk(p, z, c), loc)

    def direct(p, k):
        return copy_to(blk(p, z, c), blk(p, z, c), zsend.at[factor(p)],
                       zrecv.at[at_sem(p), z], dev(z + HOPS[k], c, me))

    def arrival(p, s):
        return copy_to(blk(p, s, c), blk(p, s, c), fsend.at[factor(p)],
                       zrecv.at[at_sem(p), s], dev(z, 1 - c, me))

    def relays(s):
        return ((s > z) & (z >= 1)) | ((s < z) & (z <= nz - 2))

    def relay(p, s):
        return copy_to(blk(p, s, c), blk(p, s, c), fsend.at[factor(p)], zrecv.at[at_sem(p), s],
                       dev(jnp.where(s > z, z - 1, z + 1), c, me))

    def landed(p, s):
        if isinstance(p, tuple):
            return urecv.at[layers - 1 + p[0]]
        return urecv.at[p // 2] if p % 2 else vrecv.at[p // 2, s]

    def push(p, s):
        return copy_to(blk(p, s, c), blk(p, s, c), psend.at[factor(p)], landed(p, s), dev(z, 1 - c, me))

    def halves(p, count):
        if isinstance(p, tuple):
            return wu.at[layers - 1, pl.ds(0, count * rs),
                         pl.ds(pl.multiple_of(p[0] * bw, bw), bw)]
        if native and p % 2 == 0:
            return wv.at[p // 2, pl.ds(0, count), :, pl.ds(0, rs)]
        return (wu if p % 2 else wv).at[p // 2, pl.ds(0, count * rs)]

    def pushed(p, s=None):
        ref = halves(p, nz) if s is None else blk(p, s, 1 - c)
        return copy_to(ref, ref, psend.at[factor(p)], landed(p, s), dev(z, 1 - c, me))

    def sent(sem, p, count):
        ref = halves(p, count)
        copy_to(ref, ref, sem.at[p], vrecv.at[0, 0], dev(z, 1 - c, me)).wait_send()

    def held(d):
        return (z >= 1) & (z <= nz - 2)

    def to_end(k):
        return (z + HOPS[k] == 0) | (z + HOPS[k] == nz - 1)

    def issue_own(p, first, k_ok=lambda k: True):
        for k in range(len(HOPS)):
            hold = held(HOPS[k])

            @pl.when(valid(HOPS[k]) & (jnp.logical_not(hold) if first else hold) & (k_ok(k)))
            def _():
                direct(p, k).start()

    def take(p, s):
        @pl.when(s != z)
        def _():
            arrival(p, s).wait_recv()

        @pl.when(relays(s))
        def _():
            relay(p, s).start()

        push(p, s).start()

    def lanes(s):
        return pl.ds(pl.multiple_of(s * ck, ck), ck)

    def seg_rows(m):
        return pl.ds(pl.multiple_of(m * seg, seg), seg)

    def other(k):
        return lax.rem(me + k, n)

    whole_in = pltpu.make_async_copy(x_ref, f_ref, in_s)
    barrier = pltpu.get_barrier_semaphore()
    for k in range(1, n):
        pl.semaphore_signal(barrier, inc=1, device_id=dev(z, c, other(k)), device_id_type=MESH)
    pl.semaphore_signal(barrier, inc=1, device_id=dev(z, 1 - c, me), device_id_type=MESH)
    for d in HOPS:
        @pl.when(valid(d))
        def _():
            pl.semaphore_signal(barrier, inc=1, device_id=dev(z + d, c, me), device_id_type=MESH)
    each_piece(lambda p: local_copy(p).start())
    whole_in.start()
    pl.semaphore_wait(barrier, n + jnp.minimum(z, 1) + jnp.minimum(nz - 1 - z, 1))

    def first_sends(p):
        issue_own(p, True)
        if p == 0:
            issue_own(p, False)
        if p == 1:
            issue_own(p, False, to_end)

    each_piece(lambda p: local_copy(p).wait())
    each_piece(first_sends)
    whole_in.wait()

    @pl.when(jnp.logical_not(end))
    def _():
        @pl.loop(0, nz)
        def _(i):
            take(0, order(i))

    if tail > 1:
        issue_own(1, False, lambda k: jnp.logical_not(to_end(k)))
    if layers > 1:
        issue_own(2, False)
    else:
        each_tail(lambda p: issue_own(p, False))

    def early(p):
        return {0: 0, 2: min(2, nz)}.get(p, 1)

    for l in range(layers):
        pv, pu = 2 * l, 2 * l + 1
        cur = f_ref if l == 0 else out_ref

        def sum_out(s, k):
            t = other(k)
            return copy_to(sbuf.at[seg_rows(t), lanes(s)], rbuf.at[l, me, :, lanes(s)],
                           rs_s, rs_r.at[s], dev(z, c, t))

        def sums_in(s):
            ref = rbuf.at[l, pl.ds(0, n - 1), :, lanes(s)]
            return copy_to(ref, ref, rs_s, rs_r.at[s], dev(z, 1 - c, me))

        def rank_out(s, k):
            mine = rank.at[l, seg_rows(me), lanes(s)]
            return copy_to(mine, mine, ag_s, ag_r, dev(z, c, other(k)))

        sums = sbuf.at[pl.ds(0, (n - 1) * seg)]
        ranks = rank.at[l, pl.ds(0, (n - 1) * seg)]
        sums_all = copy_to(sums, sums, rs_s, ag_r, dev(z, 1 - c, me))
        ranks_all = copy_to(ranks, ranks, ag_s, ag_r, dev(z, 1 - c, me))

        def reduce(s):
            acc = pf[seg_rows(me), lanes(s)]
            sums_in(s).wait_recv()
            for k in range(1, n):
                acc = acc + rbuf[l, other(k), :, lanes(s)].astype(jnp.float32)
            rank[l, seg_rows(me), lanes(s)] = acc.astype(jnp.bfloat16)
            for k in range(1, n):
                rank_out(s, k).start()

        last = l == layers - 1
        each_up = each_tail if last else lambda body: body(pu)

        @pl.loop(0, nz)
        def _(i):
            s = order(i)

            @pl.when(i == nz - 1)
            def _():
                reduce(order(i - 1))

            @pl.when(end & (i >= early(pv)))
            def _():
                take(pv, s)

            @pl.when(jnp.logical_not(end))
            def _():
                each_up(lambda p: take(p, s))

            pushed(pv, s).wait_recv()
            if native:
                part = jnp.dot(cur[...], wv[l, s], preferred_element_type=jnp.float32)
            else:
                part = lax.dot_general(cur[...], wv[l, lanes(s), :], (((1,), (1,)), ((), ())),
                                       preferred_element_type=jnp.float32)
            pf[:, lanes(s)] = part
            sbuf[:, lanes(s)] = part.astype(jnp.bfloat16)
            for k in range(1, n):
                sum_out(s, k).start()

            @pl.when((i > 0) & (i < nz - 1))
            def _():
                reduce(order(i - 1))

        if pu + 2 < tail:
            issue_own(pu + 2, False)
        elif not last and layers > 2:
            issue_own(pv + 2, False)

        reduce(order(nz - 1))

        @pl.loop(0, nz - 1)
        def _(i):
            s = order(i)

            @pl.when(end)
            def _():
                each_up(lambda p: take(p, s))

            if not last:
                @pl.when(jnp.logical_not(end))
                def _():
                    take(pv + 2, s)

        if not last:
            @pl.when(jnp.logical_not(end))
            def _():
                take(pv + 2, order(nz - 1))

            if pv + 4 < tail - 1:
                issue_own(pv + 4, False)
            elif pv + 4 > tail:
                each_tail(lambda p: issue_own(p, False))

        if last:
            @pl.when(end)
            def _():
                for p in range(tail):
                    sent(zsend, p, 1)
                    sent(psend, p, nz)
                sent(zsend, tail, 1)

        if not last:
            @pl.when(end)
            def _():
                for i in range(early(pv + 2)):
                    take(pv + 2, order(i))

        ranks_all.wait_recv()
        sums_all.wait_send()
        ranks_all.wait_send()

        if last:
            @pl.when(end)
            def _():
                take((0,), order(nz - 1))

        def finish(p):
            @pl.when(end)
            def _():
                if last:
                    @pl.when(p[0] < nb - 1)
                    def _():
                        take((p[0] + 1,), order(nz - 1))
                else:
                    take(p, order(nz - 1))

            pushed(p).wait_recv()
            width, base = (bw, p[0] * bw) if last else (cols, 0)

            @pl.loop(0, width // cb)
            def _(j):
                at = pl.ds(pl.multiple_of(base + j * cb, cb), cb)
                cross = jnp.dot(rank[l], wu[l, :, at], preferred_element_type=jnp.float32)
                cross = cross + b_ref[l, at][None, :]
                out_ref[:, at] = (f_ref[:, at].astype(jnp.float32) * cross
                                  + cur[:, at].astype(jnp.float32)).astype(jnp.bfloat16)

        each_up(finish)

    sent(psend, tail, nz)

    @pl.when(jnp.logical_not(end))
    def _():
        for p in range(tail + 1):
            sent(zsend, p, 2)
            sent(fsend, p, nz - 1)
            if p < tail:
                sent(psend, p, nz)


def solution(mesh):
    n = mesh.shape["mp"]
    nz = mesh.shape["dp"] // 2

    def local(features, v_weight, u_weight, cross_bias):
        layers, rs, cols = u_weight.shape
        rows = features.shape[0]
        r = rs * nz * 2
        nb = 8 if cols % 2048 == 0 else 1
        pieces = 2 * layers - 1 + nb
        native = rs % 128 == 0
        v = v_weight if native else jnp.swapaxes(v_weight, 1, 2)
        vm = pl.BlockSpec(memory_space=pltpu.VMEM)
        hbm = pl.BlockSpec(memory_space=pl.ANY)
        dma = pltpu.SemaphoreType.DMA
        return pl.pallas_call(
            functools.partial(kernel, nz, n, native, nb),
            out_shape=pltpu.VMEM((rows, cols), jnp.bfloat16),
            in_specs=[hbm, hbm, hbm, vm],
            out_specs=vm,
            scratch_shapes=[
                pltpu.VMEM((layers, nz, cols, 2 * rs) if native else (layers, r, cols), jnp.bfloat16),
                pltpu.VMEM((layers, r, cols), jnp.bfloat16),
                pltpu.VMEM((rows, cols), jnp.bfloat16),
                pltpu.VMEM((rows, r), jnp.float32),
                pltpu.VMEM((rows, r), jnp.bfloat16),
                pltpu.VMEM((layers, n, rows // n, r), jnp.bfloat16),
                pltpu.VMEM((layers, rows, r), jnp.bfloat16),
                dma, dma((2 * layers,)), dma((pieces, nz)), dma((2 * layers,)), dma((2 * layers,)),
                dma((layers, nz)), dma((layers - 1 + nb,)),
                dma, dma((nz,)), dma, dma, dma,
            ],
            compiler_params=pltpu.CompilerParams(
                collective_id=0, has_side_effects=True, vmem_limit_bytes=59*2**20),
            name="cross_layers",
        )(v, u_weight, features, cross_bias)

    return jax.shard_map(
        local,
        mesh=mesh,
        in_specs=(P("dp", "mp"), P(None, "mp", "dp"), P(None, "dp", "mp"), P(None, "mp")),
        out_specs=P("dp", "mp"),
        check_vma=False,
    )
```

```python
import functools

import jax
import jax.numpy as jnp
from jax import lax
from jax.experimental import pallas as pl
from jax.experimental.pallas import tpu as pltpu
from jax.sharding import PartitionSpec as P

MESH = pl.DeviceIdType.MESH
HOPS = (1, -1)
TO_Y = (0, 1, 0, 1, 1, 0, 0, 1, 1, 0)


def kernel(nz, n, native, nb, v_ref, u_ref, x_ref, b_ref, out_ref, wv, wu, f_ref, pf, sbuf, rbuf,
           rank, loc, zsend, zrecv, fsend, psend, vrecv, urecv, cbuf, rs_s, cb_s, ag_s, rs_r, cb_r, ag_r, all_r, in_s):
    layers, rs, cols = u_ref.shape
    rows = x_ref.shape[0]
    seg = rows // n
    ck = 2 * rs
    tail = 2 * layers - 1
    pieces = tail + nb
    bw = cols // nb

    def at_sem(p):
        return tail + p[0] if isinstance(p, tuple) else p

    def factor(p):
        return tail if isinstance(p, tuple) else p

    def each_tail(body):
        @pl.loop(0, nb)
        def _(b):
            body((b,))

    cb = 256 if cols % 256 == 0 else cols
    dp, me = lax.axis_index("dp"), lax.axis_index("mp")
    z, c = dp // 2, dp % 2
    step = jnp.where(2 * z < nz, 1, -1)
    end = (z == 0) | (z == nz - 1)

    def dev(zt, ct, m):
        return {"dp": zt * 2 + ct, "mp": m}

    def copy_to(src, dst, send, recv, device):
        return pltpu.make_async_remote_copy(
            src_ref=src, dst_ref=dst, send_sem=send, recv_sem=recv,
            device_id=device, device_id_type=MESH)

    def order(i):
        near = jnp.minimum(z, nz - 1 - z)
        zigzag = jnp.where(i % 2 == 1, -((i + 1) // 2), i // 2)
        return z + step * jnp.where(i <= 2 * near, zigzag, i - near)

    def valid(d):
        return (z + d >= 0) & (z + d < nz)

    def blk(p, s, cc):
        if isinstance(p, tuple):
            return wu.at[layers - 1, pl.ds(pl.multiple_of((s * 2 + cc) * rs, rs), rs),
                         pl.ds(pl.multiple_of(p[0] * bw, bw), bw)]
        if native and p % 2 == 0:
            return wv.at[p // 2, s, :, pl.ds(pl.multiple_of(cc * rs, rs), rs)]
        w = wu if p % 2 else wv
        return w.at[p // 2, pl.ds(pl.multiple_of((s * 2 + cc) * rs, rs), rs)]

    def local_copy(p):
        if isinstance(p, tuple):
            src = u_ref.at[layers - 1, :, pl.ds(pl.multiple_of(p[0] * bw, bw), bw)]
        else:
            src = (v_ref if p % 2 == 0 else u_ref).at[p // 2]
        return pltpu.make_async_copy(src, blk(p, z, c), loc.at[0 if p == 0 else 1])

    def direct(p, k):
        return copy_to(blk(p, z, c), blk(p, z, c), zsend.at[factor(p)],
                       zrecv.at[at_sem(p), z], dev(z + HOPS[k], c, me))

    def arrival(p, s):
        return copy_to(blk(p, s, c), blk(p, s, c), fsend.at[factor(p)],
                       zrecv.at[at_sem(p), s], dev(z, 1 - c, me))

    def relays(s):
        return ((s > z) & (z >= 1)) | ((s < z) & (z <= nz - 2))

    def relay(p, s):
        return copy_to(blk(p, s, c), blk(p, s, c), fsend.at[factor(p)], zrecv.at[at_sem(p), s],
                       dev(jnp.where(s > z, z - 1, z + 1), c, me))

    def landed(p, s):
        if isinstance(p, tuple):
            return urecv.at[layers - 1 + p[0]]
        return urecv.at[p // 2] if p % 2 else vrecv.at[p // 2, s]

    def push(p, s):
        return copy_to(blk(p, s, c), blk(p, s, c), psend.at[factor(p)], landed(p, s), dev(z, 1 - c, me))

    def halves(p, count):
        if isinstance(p, tuple):
            return wu.at[layers - 1, pl.ds(0, count * rs),
                         pl.ds(pl.multiple_of(p[0] * bw, bw), bw)]
        if native and p % 2 == 0:
            return wv.at[p // 2, pl.ds(0, count), :, pl.ds(0, rs)]
        return (wu if p % 2 else wv).at[p // 2, pl.ds(0, count * rs)]

    def pushed(p, s=None):
        ref = halves(p, nz) if s is None else blk(p, s, 1 - c)
        return copy_to(ref, ref, psend.at[factor(p)], landed(p, s), dev(z, 1 - c, me))

    def sent(sem, p, count):
        ref = halves(p, count)
        copy_to(ref, ref, sem.at[p], vrecv.at[0, 0], dev(z, 1 - c, me)).wait_send()

    def held(d):
        return (z >= 1) & (z <= nz - 2)

    def to_end(k):
        return (z + HOPS[k] == 0) | (z + HOPS[k] == nz - 1)

    def issue_own(p, first, k_ok=lambda k: True):
        for k in range(len(HOPS)):
            hold = held(HOPS[k])

            @pl.when(valid(HOPS[k]) & (jnp.logical_not(hold) if first else hold) & (k_ok(k)))
            def _():
                direct(p, k).start()

    def take(p, s):
        @pl.when(s != z)
        def _():
            arrival(p, s).wait_recv()

        @pl.when(relays(s))
        def _():
            relay(p, s).start()

        push(p, s).start()

    def lanes(s):
        return pl.ds(pl.multiple_of(s * ck, ck), ck)

    def seg_rows(m):
        return pl.ds(pl.multiple_of(m * seg, seg), seg)

    def half(m, h):
        return pl.ds(pl.multiple_of(m * seg + h * (seg // 2), seg // 2), seg // 2)

    two = n == 4
    peers = (me + 1 - 2 * (me % 2), lax.rem(me + 2, n), n - 1 - me, me)

    def other(k):
        return lax.rem(me + k, n)

    whole_in = pltpu.make_async_copy(x_ref, f_ref, in_s)
    barrier = pltpu.get_barrier_semaphore()
    for m in peers[:2] if two else [other(k) for k in range(1, n)]:
        pl.semaphore_signal(barrier, inc=1, device_id=dev(z, c, m), device_id_type=MESH)
    pl.semaphore_signal(barrier, inc=1, device_id=dev(z, 1 - c, me), device_id_type=MESH)
    for d in HOPS:
        @pl.when(valid(d))
        def _():
            pl.semaphore_signal(barrier, inc=1, device_id=dev(z + d, c, me), device_id_type=MESH)
    local_copy(0).start()
    pl.semaphore_wait(barrier, (3 if two else n) + jnp.minimum(z, 1) + jnp.minimum(nz - 1 - z, 1))

    def first_sends(p):
        issue_own(p, True)
        if p == 0:
            issue_own(p, False)
        if p == 1:
            issue_own(p, False, to_end)

    def rest(body):
        for p in range(1, tail):
            body(p)
        each_tail(body)

    local_copy(0).wait()
    first_sends(0)
    rest(lambda p: local_copy(p).start())
    whole_in.start()
    rest(lambda p: local_copy(p).wait())
    rest(first_sends)
    whole_in.wait()

    @pl.when(jnp.logical_not(end))
    def _():
        @pl.loop(0, nz)
        def _(i):
            take(0, order(i))

    if tail > 1:
        issue_own(1, False, lambda k: jnp.logical_not(to_end(k)))
    if layers > 1:
        issue_own(2, False)
    else:
        each_tail(lambda p: issue_own(p, False))

    def early(p):
        return {0: 0, 2: min(2, nz)}.get(p, 1)

    for l in range(layers):
        pv, pu = 2 * l, 2 * l + 1
        cur = f_ref if l == 0 else out_ref

        def sum_out(s, k):
            t = other(k)
            return copy_to(sbuf.at[seg_rows(t), lanes(s)], rbuf.at[l, me, :, lanes(s)],
                           rs_s, rs_r.at[s], dev(z, c, t))

        def sums_in(s):
            ref = rbuf.at[l, pl.ds(0, n - 1), :, lanes(s)]
            return copy_to(ref, ref, rs_s, rs_r.at[s], dev(z, 1 - c, me))

        def rank_out(s, k):
            mine = rank.at[l, seg_rows(me), lanes(s)]
            return copy_to(mine, mine, ag_s, all_r, dev(z, c, other(k)))

        def reduce(s):
            acc = pf[seg_rows(me), lanes(s)]
            sums_in(s).wait_recv()
            for k in range(1, n):
                acc = acc + rbuf[l, other(k), :, lanes(s)].astype(jnp.float32)
            rank[l, seg_rows(me), lanes(s)] = acc.astype(jnp.bfloat16)
            for k in range(1, n):
                rank_out(s, k).start()

        def mp_refs(kind, s):
            at, here = lanes(s), rbuf.at[l, min(kind, 5), :, lanes(s)]
            if kind < 4:
                rows_at = half(peers[(2, 2, 0, 1)[kind]], (0, 1, 0, 1)[kind])
                return sbuf.at[rows_at, at], here, rs_s, (rs_r if kind < 2 else cb_r).at[s]
            if kind < 6:
                return cbuf.at[kind - 4, :, at], here, cb_s, cb_r.at[s]
            mine = (seg_rows(me), seg_rows(me), half(peers[0], 0), half(peers[1], 1))[kind - 6]
            ref = rank.at[l, mine, at]
            return ref, ref, ag_s, ag_r.at[s] if kind < 8 else all_r

        def mp_out(kind, s):
            src, dst, send, recv = mp_refs(kind, s)
            return copy_to(src, dst, send, recv, dev(z, c, peers[TO_Y[kind]]))

        def got(ref, sem):
            copy_to(ref, ref, rs_s, sem, dev(z, 1 - c, me)).wait_recv()

        def gone(ref, sem):
            copy_to(ref, ref, sem, all_r, dev(z, 1 - c, me)).wait_send()

        def sum_on(s):
            at = lanes(s)
            got(rbuf.at[l, pl.ds(0, 2), :, at], rs_r.at[s])
            for h in range(2):
                cbuf[h, :, at] = (pf[half(peers[1 - h], h), at]
                                  + rbuf[l, h, :, at].astype(jnp.float32)).astype(jnp.bfloat16)
                mp_out(4 + h, s).start()

        def sum_up(s):
            at = lanes(s)
            got(rbuf.at[l, pl.ds(2, 4), :, at], cb_r.at[s])
            for h in range(2):
                acc = pf[half(me, h), at] + rbuf[l, 2 + h, :, at].astype(jnp.float32)
                acc = acc + rbuf[l, 4 + h, :, at].astype(jnp.float32)
                rank[l, half(me, h), at] = acc.astype(jnp.bfloat16)
            for kind in (6, 7):
                mp_out(kind, s).start()

        def pass_on(s):
            got(rank.at[l, pl.ds(0, 2 * seg), lanes(s)], ag_r.at[s])
            for kind in (8, 9):
                mp_out(kind, s).start()

        def exchange(i, stages):
            for lag, stage in stages:
                @pl.when((i >= lag) & (i < nz + lag))
                def _():
                    stage(order(i - lag))

        steps = ((1, sum_on), (2, sum_up), (3, pass_on)) if two else ((1, reduce),)

        last = l == layers - 1
        each_up = each_tail if last else lambda body: body(pu)

        @pl.loop(0, nz)
        def _(i):
            s = order(i)

            if two:
                exchange(i, steps)
            else:
                @pl.when(i == nz - 1)
                def _():
                    reduce(order(i - 1))

            @pl.when(end & (i >= early(pv)))
            def _():
                take(pv, s)

            @pl.when(jnp.logical_not(end))
            def _():
                each_up(lambda p: take(p, s))

            pushed(pv, s).wait_recv()
            if native:
                part = jnp.dot(cur[...], wv[l, s], preferred_element_type=jnp.float32)
            else:
                part = lax.dot_general(cur[...], wv[l, lanes(s), :], (((1,), (1,)), ((), ())),
                                       preferred_element_type=jnp.float32)
            pf[:, lanes(s)] = part
            sbuf[:, lanes(s)] = part.astype(jnp.bfloat16)
            if two:
                for kind in range(4):
                    mp_out(kind, s).start()
            else:
                for k in range(1, n):
                    sum_out(s, k).start()

                @pl.when((i > 0) & (i < nz - 1))
                def _():
                    reduce(order(i - 1))

        if pu + 2 < tail:
            issue_own(pu + 2, False)
        elif not last and layers > 2:
            issue_own(pv + 2, False)

        if two:
            @pl.loop(nz, nz + 3)
            def _(i):
                exchange(i, steps)
        else:
            reduce(order(nz - 1))

        @pl.loop(0, nz - 1)
        def _(i):
            s = order(i)

            @pl.when(end)
            def _():
                each_up(lambda p: take(p, s))

            if not last:
                @pl.when(jnp.logical_not(end))
                def _():
                    take(pv + 2, s)

        if not last:
            @pl.when(jnp.logical_not(end))
            def _():
                take(pv + 2, order(nz - 1))

            if pv + 4 < tail - 1:
                issue_own(pv + 4, False)
            elif pv + 4 > tail:
                each_tail(lambda p: issue_own(p, False))

        if last:
            @pl.when(end)
            def _():
                for p in range(tail):
                    sent(zsend, p, 1)
                    sent(psend, p, nz)
                sent(zsend, tail, 1)

        if not last:
            @pl.when(end)
            def _():
                for i in range(early(pv + 2)):
                    take(pv + 2, order(i))

        if two:
            got(rank.at[l, pl.ds(0, seg)], all_r)
            gone(sbuf.at[pl.ds(0, 2 * seg)], rs_s)
            gone(cbuf, cb_s)
            gone(rank.at[l, pl.ds(0, 3 * seg)], ag_s)
        else:
            got(rank.at[l, pl.ds(0, (n - 1) * seg)], all_r)
            gone(sbuf.at[pl.ds(0, (n - 1) * seg)], rs_s)
            gone(rank.at[l, pl.ds(0, (n - 1) * seg)], ag_s)

        if last:
            @pl.when(end)
            def _():
                take((0,), order(nz - 1))

        def finish(p):
            @pl.when(end)
            def _():
                if last:
                    @pl.when(p[0] < nb - 1)
                    def _():
                        take((p[0] + 1,), order(nz - 1))
                else:
                    take(p, order(nz - 1))

            pushed(p).wait_recv()
            width, base = (bw, p[0] * bw) if last else (cols, 0)

            @pl.loop(0, width // cb)
            def _(j):
                at = pl.ds(pl.multiple_of(base + j * cb, cb), cb)
                cross = jnp.dot(rank[l], wu[l, :, at], preferred_element_type=jnp.float32)
                cross = cross + b_ref[l, at][None, :]
                out_ref[:, at] = (f_ref[:, at].astype(jnp.float32) * cross
                                  + cur[:, at].astype(jnp.float32)).astype(jnp.bfloat16)

        each_up(finish)

    sent(psend, tail, nz)

    @pl.when(jnp.logical_not(end))
    def _():
        for p in range(tail + 1):
            sent(zsend, p, 2)
            sent(fsend, p, nz - 1)
            if p < tail:
                sent(psend, p, nz)


def solution(mesh):
    n = mesh.shape["mp"]
    nz = mesh.shape["dp"] // 2

    def local(features, v_weight, u_weight, cross_bias):
        layers, rs, cols = u_weight.shape
        rows = features.shape[0]
        r = rs * nz * 2
        nb = 8 if cols % 2048 == 0 else 1
        pieces = 2 * layers - 1 + nb
        native = rs % 128 == 0
        v = v_weight if native else jnp.swapaxes(v_weight, 1, 2)
        vm = pl.BlockSpec(memory_space=pltpu.VMEM)
        hbm = pl.BlockSpec(memory_space=pl.ANY)
        dma = pltpu.SemaphoreType.DMA
        return pl.pallas_call(
            functools.partial(kernel, nz, n, native, nb),
            out_shape=pltpu.VMEM((rows, cols), jnp.bfloat16),
            in_specs=[hbm, hbm, hbm, vm],
            out_specs=vm,
            scratch_shapes=[
                pltpu.VMEM((layers, nz, cols, 2 * rs) if native else (layers, r, cols), jnp.bfloat16),
                pltpu.VMEM((layers, r, cols), jnp.bfloat16),
                pltpu.VMEM((rows, cols), jnp.bfloat16),
                pltpu.VMEM((rows, r), jnp.float32),
                pltpu.VMEM((rows, r), jnp.bfloat16),
                pltpu.VMEM((layers, 6, rows // (2 * n), r) if n == 4 else (layers, n, rows // n, r),
                           jnp.bfloat16),
                pltpu.VMEM((layers, rows, r), jnp.bfloat16),
                dma((2,)), dma((2 * layers,)), dma((pieces, nz)), dma((2 * layers,)), dma((2 * layers,)),
                dma((layers, nz)), dma((layers - 1 + nb,)),
                pltpu.VMEM((2, rows // (2 * n), r), jnp.bfloat16),
                dma, dma, dma, dma((nz,)), dma((nz,)), dma((nz,)), dma, dma,
            ],
            compiler_params=pltpu.CompilerParams(
                collective_id=0, has_side_effects=True, vmem_limit_bytes=59*2**20),
            name="cross_layers",
        )(v, u_weight, features, cross_bias)

    return jax.shard_map(
        local,
        mesh=mesh,
        in_specs=(P("dp", "mp"), P(None, "mp", "dp"), P(None, "dp", "mp"), P(None, "mp")),
        out_specs=P("dp", "mp"),
        check_vma=False,
    )
```

```python
import functools

import jax
import jax.numpy as jnp
from jax import lax
from jax.experimental import pallas as pl
from jax.experimental.pallas import tpu as pltpu
from jax.sharding import PartitionSpec as P

MESH = pl.DeviceIdType.MESH
HOPS = (1, -1)
TO_Y = (0, 1, 0, 1, 1, 0, 0, 1, 1, 0)


def kernel(nz, n, native, nb, v_ref, u_ref, x_ref, b_ref, out_ref, rank_ref, last_ref, kept_ref, wv, wu, f_ref, pf, sbuf, rbuf,
           rank, loc, zsend, zrecv, fsend, psend, vrecv, urecv, cbuf, rs_s, cb_s, ag_s, rs_r, cb_r, ag_r, all_r, in_s):
    layers, rs, cols = u_ref.shape
    rows = x_ref.shape[0]
    seg = rows // n
    ck = 2 * rs
    tail = 2 * layers - 1
    pieces = tail + nb
    bw = cols // nb

    def at_sem(p):
        if p is final:
            return tail + nb - 1
        return tail + p[0] if isinstance(p, tuple) else p

    def factor(p):
        return tail if isinstance(p, tuple) else p

    final = (None,)

    def each_tail(body):
        @pl.loop(0, nb - 1)
        def _(b):
            body((b,))

        body(final)

    cb = 256 if cols % 256 == 0 else cols
    dp, me = lax.axis_index("dp"), lax.axis_index("mp")
    z, c = dp // 2, dp % 2
    step = jnp.where(2 * z < nz, 1, -1)
    end = (z == 0) | (z == nz - 1)

    def dev(zt, ct, m):
        return {"dp": zt * 2 + ct, "mp": m}

    def copy_to(src, dst, send, recv, device):
        return pltpu.make_async_remote_copy(
            src_ref=src, dst_ref=dst, send_sem=send, recv_sem=recv,
            device_id=device, device_id_type=MESH)

    def order(i):
        near = jnp.minimum(z, nz - 1 - z)
        zigzag = jnp.where(i % 2 == 1, -((i + 1) // 2), i // 2)
        return z + step * jnp.where(i <= 2 * near, zigzag, i - near)

    def valid(d):
        return (z + d >= 0) & (z + d < nz)

    def blk(p, s, cc):
        if p is final:
            return last_ref.at[pl.ds(pl.multiple_of((s * 2 + cc) * rs, rs), rs)]
        if isinstance(p, tuple):
            return wu.at[layers - 1, pl.ds(pl.multiple_of((s * 2 + cc) * rs, rs), rs),
                         pl.ds(pl.multiple_of(p[0] * bw, bw), bw)]
        if native and p % 2 == 0:
            return wv.at[p // 2, s, :, pl.ds(pl.multiple_of(cc * rs, rs), rs)]
        w = wu if p % 2 else wv
        return w.at[p // 2, pl.ds(pl.multiple_of((s * 2 + cc) * rs, rs), rs)]

    def local_copy(p):
        if p is final:
            src = u_ref.at[layers - 1, :, pl.ds(cols - bw, bw)]
        elif isinstance(p, tuple):
            src = u_ref.at[layers - 1, :, pl.ds(pl.multiple_of(p[0] * bw, bw), bw)]
        else:
            src = (v_ref if p % 2 == 0 else u_ref).at[p // 2]
        return pltpu.make_async_copy(src, blk(p, z, c), loc.at[0 if p == 0 else 1])

    def direct(p, k):
        return copy_to(blk(p, z, c), blk(p, z, c), zsend.at[factor(p)],
                       zrecv.at[at_sem(p), z], dev(z + HOPS[k], c, me))

    def arrival(p, s):
        return copy_to(blk(p, s, c), blk(p, s, c), fsend.at[factor(p)],
                       zrecv.at[at_sem(p), s], dev(z, 1 - c, me))

    def relays(s):
        return ((s > z) & (z >= 1)) | ((s < z) & (z <= nz - 2))

    def relay(p, s):
        return copy_to(blk(p, s, c), blk(p, s, c), fsend.at[factor(p)], zrecv.at[at_sem(p), s],
                       dev(jnp.where(s > z, z - 1, z + 1), c, me))

    def landed(p, s):
        if isinstance(p, tuple):
            return urecv.at[layers - 1 + (nb - 1 if p is final else p[0])]
        return urecv.at[p // 2] if p % 2 else vrecv.at[p // 2, s]

    def push(p, s):
        return copy_to(blk(p, s, c), blk(p, s, c), psend.at[factor(p)], landed(p, s), dev(z, 1 - c, me))

    def halves(p, count):
        if p is final:
            return last_ref.at[pl.ds(0, count * rs)]
        if isinstance(p, tuple):
            return wu.at[layers - 1, pl.ds(0, count * rs),
                         pl.ds(pl.multiple_of(p[0] * bw, bw), bw)]
        if native and p % 2 == 0:
            return wv.at[p // 2, pl.ds(0, count), :, pl.ds(0, rs)]
        return (wu if p % 2 else wv).at[p // 2, pl.ds(0, count * rs)]

    def pushed(p, s=None):
        ref = halves(p, nz) if s is None else blk(p, s, 1 - c)
        return copy_to(ref, ref, psend.at[factor(p)], landed(p, s), dev(z, 1 - c, me))

    def sent(sem, p, count):
        ref = halves(p, count)
        copy_to(ref, ref, sem.at[p], vrecv.at[0, 0], dev(z, 1 - c, me)).wait_send()

    def held(d):
        return (z >= 1) & (z <= nz - 2)

    def to_end(k):
        return (z + HOPS[k] == 0) | (z + HOPS[k] == nz - 1)

    def issue_own(p, first, k_ok=lambda k: True):
        for k in range(len(HOPS)):
            hold = held(HOPS[k])

            @pl.when(valid(HOPS[k]) & (jnp.logical_not(hold) if first else hold) & (k_ok(k)))
            def _():
                direct(p, k).start()

    def take(p, s):
        @pl.when(s != z)
        def _():
            arrival(p, s).wait_recv()

        @pl.when(relays(s))
        def _():
            relay(p, s).start()

        push(p, s).start()

    def lanes(s):
        return pl.ds(pl.multiple_of(s * ck, ck), ck)

    def seg_rows(m):
        return pl.ds(pl.multiple_of(m * seg, seg), seg)

    def half(m, h):
        return pl.ds(pl.multiple_of(m * seg + h * (seg // 2), seg // 2), seg // 2)

    two = n == 4
    peers = (me + 1 - 2 * (me % 2), lax.rem(me + 2, n), n - 1 - me, me)

    def other(k):
        return lax.rem(me + k, n)

    whole_in = pltpu.make_async_copy(x_ref, f_ref, in_s)
    barrier = pltpu.get_barrier_semaphore()
    for m in peers[:2] if two else [other(k) for k in range(1, n)]:
        pl.semaphore_signal(barrier, inc=1, device_id=dev(z, c, m), device_id_type=MESH)
    pl.semaphore_signal(barrier, inc=1, device_id=dev(z, 1 - c, me), device_id_type=MESH)
    for d in HOPS:
        @pl.when(valid(d))
        def _():
            pl.semaphore_signal(barrier, inc=1, device_id=dev(z + d, c, me), device_id_type=MESH)
    local_copy(0).start()
    pl.semaphore_wait(barrier, (3 if two else n) + jnp.minimum(z, 1) + jnp.minimum(nz - 1 - z, 1))

    def first_sends(p):
        issue_own(p, True)
        if p == 0:
            issue_own(p, False)
        if p == 1:
            issue_own(p, False, to_end)

    def rest(body):
        for p in range(1, tail):
            body(p)
        each_tail(body)

    local_copy(0).wait()
    first_sends(0)
    rest(lambda p: local_copy(p).start())
    whole_in.start()
    rest(lambda p: local_copy(p).wait())
    rest(first_sends)
    whole_in.wait()
    kept_ref[...] = f_ref[:, pl.ds(cols - bw, bw)]

    @pl.when(jnp.logical_not(end))
    def _():
        @pl.loop(0, nz)
        def _(i):
            take(0, order(i))

    if tail > 1:
        issue_own(1, False, lambda k: jnp.logical_not(to_end(k)))
    if layers > 1:
        issue_own(2, False)
    else:
        each_tail(lambda p: issue_own(p, False))

    def early(p):
        return {0: 0, 2: min(2, nz)}.get(p, 1)

    for l in range(layers):
        pv, pu = 2 * l, 2 * l + 1
        cur = f_ref if l == 0 else out_ref
        last = l == layers - 1
        rk = rank_ref if last else rank.at[l]

        def sum_out(s, k):
            t = other(k)
            return copy_to(sbuf.at[seg_rows(t), lanes(s)], rbuf.at[l, me, :, lanes(s)],
                           rs_s, rs_r.at[s], dev(z, c, t))

        def sums_in(s):
            ref = rbuf.at[l, pl.ds(0, n - 1), :, lanes(s)]
            return copy_to(ref, ref, rs_s, rs_r.at[s], dev(z, 1 - c, me))

        def rank_out(s, k):
            mine = rk.at[seg_rows(me), lanes(s)]
            return copy_to(mine, mine, ag_s, all_r, dev(z, c, other(k)))

        def reduce(s):
            acc = pf[seg_rows(me), lanes(s)]
            sums_in(s).wait_recv()
            for k in range(1, n):
                acc = acc + rbuf[l, other(k), :, lanes(s)].astype(jnp.float32)
            rk[seg_rows(me), lanes(s)] = acc.astype(jnp.bfloat16)
            for k in range(1, n):
                rank_out(s, k).start()

        def mp_refs(kind, s):
            at, here = lanes(s), rbuf.at[l, min(kind, 5), :, lanes(s)]
            if kind < 4:
                rows_at = half(peers[(2, 2, 0, 1)[kind]], (0, 1, 0, 1)[kind])
                return sbuf.at[rows_at, at], here, rs_s, (rs_r if kind < 2 else cb_r).at[s]
            if kind < 6:
                return cbuf.at[kind - 4, :, at], here, cb_s, cb_r.at[s]
            mine = (seg_rows(me), seg_rows(me), half(peers[0], 0), half(peers[1], 1))[kind - 6]
            ref = rk.at[mine, at]
            return ref, ref, ag_s, ag_r.at[s] if kind < 8 else all_r

        def mp_out(kind, s):
            src, dst, send, recv = mp_refs(kind, s)
            return copy_to(src, dst, send, recv, dev(z, c, peers[TO_Y[kind]]))

        def got(ref, sem):
            copy_to(ref, ref, rs_s, sem, dev(z, 1 - c, me)).wait_recv()

        def gone(ref, sem):
            copy_to(ref, ref, sem, all_r, dev(z, 1 - c, me)).wait_send()

        def sum_on(s):
            at = lanes(s)
            got(rbuf.at[l, pl.ds(0, 2), :, at], rs_r.at[s])
            for h in range(2):
                cbuf[h, :, at] = (pf[half(peers[1 - h], h), at]
                                  + rbuf[l, h, :, at].astype(jnp.float32)).astype(jnp.bfloat16)
                mp_out(4 + h, s).start()

        def sum_up(s):
            at = lanes(s)
            got(rbuf.at[l, pl.ds(2, 4), :, at], cb_r.at[s])
            for h in range(2):
                acc = pf[half(me, h), at] + rbuf[l, 2 + h, :, at].astype(jnp.float32)
                acc = acc + rbuf[l, 4 + h, :, at].astype(jnp.float32)
                rk[half(me, h), at] = acc.astype(jnp.bfloat16)
            for kind in (6, 7):
                mp_out(kind, s).start()

        def pass_on(s):
            got(rk.at[pl.ds(0, 2 * seg), lanes(s)], ag_r.at[s])
            for kind in (8, 9):
                mp_out(kind, s).start()

        def exchange(i, stages):
            for lag, stage in stages:
                @pl.when((i >= lag) & (i < nz + lag))
                def _():
                    stage(order(i - lag))

        steps = ((1, sum_on), (2, sum_up), (3, pass_on)) if two else ((1, reduce),)

        each_up = each_tail if last else lambda body: body(pu)

        @pl.loop(0, nz)
        def _(i):
            s = order(i)

            if two:
                exchange(i, steps)
            else:
                @pl.when(i == nz - 1)
                def _():
                    reduce(order(i - 1))

            @pl.when(end & (i >= early(pv)))
            def _():
                take(pv, s)

            @pl.when(jnp.logical_not(end))
            def _():
                each_up(lambda p: take(p, s))

            pushed(pv, s).wait_recv()
            if native:
                part = jnp.dot(cur[...], wv[l, s], preferred_element_type=jnp.float32)
            else:
                part = lax.dot_general(cur[...], wv[l, lanes(s), :], (((1,), (1,)), ((), ())),
                                       preferred_element_type=jnp.float32)
            pf[:, lanes(s)] = part
            sbuf[:, lanes(s)] = part.astype(jnp.bfloat16)
            if two:
                for kind in range(4):
                    mp_out(kind, s).start()
            else:
                for k in range(1, n):
                    sum_out(s, k).start()

                @pl.when((i > 0) & (i < nz - 1))
                def _():
                    reduce(order(i - 1))

        if pu + 2 < tail:
            issue_own(pu + 2, False)
        elif not last and layers > 2:
            issue_own(pv + 2, False)

        if two:
            @pl.loop(nz, nz + 3)
            def _(i):
                exchange(i, steps)
        else:
            reduce(order(nz - 1))

        @pl.loop(0, nz - 1)
        def _(i):
            s = order(i)

            @pl.when(end)
            def _():
                each_up(lambda p: take(p, s))

            if not last:
                @pl.when(jnp.logical_not(end))
                def _():
                    take(pv + 2, s)

        if not last:
            @pl.when(jnp.logical_not(end))
            def _():
                take(pv + 2, order(nz - 1))

            if pv + 4 < tail - 1:
                issue_own(pv + 4, False)
            elif pv + 4 > tail:
                each_tail(lambda p: issue_own(p, False))

        if last:
            @pl.when(end)
            def _():
                for p in range(tail):
                    sent(zsend, p, 1)
                    sent(psend, p, nz)
                sent(zsend, tail, 1)

        if not last:
            @pl.when(end)
            def _():
                for i in range(early(pv + 2)):
                    take(pv + 2, order(i))

        if two:
            got(rk.at[pl.ds(0, seg)], all_r)
            gone(sbuf.at[pl.ds(0, 2 * seg)], rs_s)
            gone(cbuf, cb_s)
            gone(rk.at[pl.ds(0, 3 * seg)], ag_s)
        else:
            got(rk.at[pl.ds(0, (n - 1) * seg)], all_r)
            gone(sbuf.at[pl.ds(0, (n - 1) * seg)], rs_s)
            gone(rk.at[pl.ds(0, (n - 1) * seg)], ag_s)

        if last:
            @pl.when(end)
            def _():
                take((0,) if nb > 1 else final, order(nz - 1))

        def finish(p):
            @pl.when(end)
            def _():
                if last:
                    if p is not final:
                        @pl.when(p[0] < nb - 2)
                        def _():
                            take((p[0] + 1,), order(nz - 1))

                        @pl.when(p[0] == nb - 2)
                        def _():
                            take(final, order(nz - 1))
                else:
                    take(p, order(nz - 1))

            pushed(p).wait_recv()
            if p is final:
                return
            width, base = (bw, p[0] * bw) if last else (cols, 0)

            @pl.loop(0, width // cb)
            def _(j):
                at = pl.ds(pl.multiple_of(base + j * cb, cb), cb)
                cross = jnp.dot(rk[...], wu[l, :, at], preferred_element_type=jnp.float32)
                cross = cross + b_ref[l, at][None, :]
                out_ref[:, at] = (f_ref[:, at].astype(jnp.float32) * cross
                                  + cur[:, at].astype(jnp.float32)).astype(jnp.bfloat16)

        each_up(finish)

    sent(psend, tail, nz)

    @pl.when(jnp.logical_not(end))
    def _():
        for p in range(tail + 1):
            sent(zsend, p, 2)
            sent(fsend, p, nz - 1)
            if p < tail:
                sent(psend, p, nz)


def last_block(x_ref, rank_ref, u_ref, b_ref, f_ref, y_ref, block, sems):
    cols, bw = x_ref.shape[1], u_ref.shape[1]
    done, at = pl.ds(0, cols - bw), pl.ds(cols - bw, bw)
    store = pltpu.make_async_copy(block, y_ref.at[:, at], sems.at[0])
    if cols > bw:
        ready = pltpu.make_async_copy(x_ref.at[:, done], y_ref.at[:, done], sems.at[1])
        ready.start()
    cross = jnp.dot(rank_ref[...], u_ref[...], preferred_element_type=jnp.float32)
    cross = cross + b_ref[b_ref.shape[0] - 1, at][None, :]
    block[...] = (f_ref[...].astype(jnp.float32) * cross
                  + x_ref[:, at].astype(jnp.float32)).astype(jnp.bfloat16)
    store.start()
    if cols > bw:
        ready.wait()
    store.wait()


def solution(mesh):
    n = mesh.shape["mp"]
    nz = mesh.shape["dp"] // 2

    def local(features, v_weight, u_weight, cross_bias):
        layers, rs, cols = u_weight.shape
        rows = features.shape[0]
        r = rs * nz * 2
        nb = cols // 256 if cols % 256 == 0 else 1
        pieces = 2 * layers - 1 + nb
        native = rs % 128 == 0
        v = v_weight if native else jnp.swapaxes(v_weight, 1, 2)
        vm = pl.BlockSpec(memory_space=pltpu.VMEM)
        hbm = pl.BlockSpec(memory_space=pl.ANY)
        dma = pltpu.SemaphoreType.DMA
        crossed, rank, u_last, kept = pl.pallas_call(
            functools.partial(kernel, nz, n, native, nb),
            out_shape=(pltpu.VMEM((rows, cols), jnp.bfloat16), pltpu.VMEM((rows, r), jnp.bfloat16),
                       pltpu.VMEM((r, cols // nb), jnp.bfloat16),
                       pltpu.VMEM((rows, cols // nb), jnp.bfloat16)),
            in_specs=[hbm, hbm, hbm, vm],
            out_specs=(vm, vm, vm, vm),
            scratch_shapes=[
                pltpu.VMEM((layers, nz, cols, 2 * rs) if native else (layers, r, cols), jnp.bfloat16),
                pltpu.VMEM((layers, r, cols), jnp.bfloat16),
                pltpu.VMEM((rows, cols), jnp.bfloat16),
                pltpu.VMEM((rows, r), jnp.float32),
                pltpu.VMEM((rows, r), jnp.bfloat16),
                pltpu.VMEM((layers, 6, rows // (2 * n), r) if n == 4 else (layers, n, rows // n, r),
                           jnp.bfloat16),
                pltpu.VMEM((max(layers - 1, 1), rows, r), jnp.bfloat16),
                dma((2,)), dma((2 * layers,)), dma((pieces, nz)), dma((2 * layers,)), dma((2 * layers,)),
                dma((layers, nz)), dma((layers - 1 + nb,)),
                pltpu.VMEM((2, rows // (2 * n), r), jnp.bfloat16),
                dma, dma, dma, dma((nz,)), dma((nz,)), dma((nz,)), dma, dma,
            ],
            compiler_params=pltpu.CompilerParams(
                collective_id=0, has_side_effects=True, vmem_limit_bytes=55 * 2**20),
            name="cross_layers",
        )(v, u_weight, features, cross_bias)
        return pl.pallas_call(
            last_block,
            out_shape=jax.ShapeDtypeStruct((rows, cols), jnp.bfloat16),
            in_specs=[vm, vm, vm, vm, vm],
            out_specs=hbm,
            scratch_shapes=[pltpu.VMEM((rows, cols // nb), jnp.bfloat16), dma((2,))],
            compiler_params=pltpu.CompilerParams(vmem_limit_bytes=16 * 2**20),
            name="last_block",
        )(crossed, rank, u_last, cross_bias, kept)

    return jax.shard_map(
        local,
        mesh=mesh,
        in_specs=(P("dp", "mp"), P(None, "mp", "dp"), P(None, "dp", "mp"), P(None, "mp")),
        out_specs=P("dp", "mp"),
        check_vma=False,
    )
```

```python
import functools

import jax
import jax.numpy as jnp
from jax import lax
from jax.experimental import pallas as pl
from jax.experimental.pallas import tpu as pltpu
from jax.sharding import PartitionSpec as P

MESH = pl.DeviceIdType.MESH
HOPS = (1, -1)
TO_Y = (0, 1, 0, 1, 1, 0, 0, 1, 1, 0)


def kernel(nz, n, native, nb, v_ref, u_ref, x_ref, b_ref, out_ref, rank_ref, last_ref, kept_ref, wv, wu, f_ref, pf, sbuf, rbuf,
           rank, loc, zsend, zrecv, fsend, psend, vrecv, urecv, cbuf, rs_s, cb_s, ag_s, rs_r, cb_r, ag_r, all_r, in_s):
    layers, rs, cols = u_ref.shape
    rows = x_ref.shape[0]
    seg = rows // n
    ck = 2 * rs
    tail = 2 * layers - 1
    pieces = tail + nb
    bw = cols // nb

    def at_sem(p):
        if p is final:
            return tail + nb - 1
        return tail + p[0] if isinstance(p, tuple) else p

    def factor(p):
        return tail if isinstance(p, tuple) else p

    final = (None,)

    def each_tail(body):
        @pl.loop(0, nb - 1)
        def _(b):
            body((b,))

        body(final)

    cb = 256 if cols % 256 == 0 else cols
    dp, me = lax.axis_index("dp"), lax.axis_index("mp")
    z, c = dp // 2, dp % 2
    step = jnp.where(2 * z < nz, 1, -1)
    end = (z == 0) | (z == nz - 1)

    def dev(zt, ct, m):
        return {"dp": zt * 2 + ct, "mp": m}

    def copy_to(src, dst, send, recv, device):
        return pltpu.make_async_remote_copy(
            src_ref=src, dst_ref=dst, send_sem=send, recv_sem=recv,
            device_id=device, device_id_type=MESH)

    def order(i):
        near = jnp.minimum(z, nz - 1 - z)
        zigzag = jnp.where(i % 2 == 1, -((i + 1) // 2), i // 2)
        return z + step * jnp.where(i <= 2 * near, zigzag, i - near)

    def valid(d):
        return (z + d >= 0) & (z + d < nz)

    def blk(p, s, cc):
        if p is final:
            return last_ref.at[pl.ds(pl.multiple_of((s * 2 + cc) * rs, rs), rs)]
        if isinstance(p, tuple):
            return wu.at[layers - 1, pl.ds(pl.multiple_of((s * 2 + cc) * rs, rs), rs),
                         pl.ds(pl.multiple_of(p[0] * bw, bw), bw)]
        if native and p % 2 == 0:
            return wv.at[p // 2, s, :, pl.ds(pl.multiple_of(cc * rs, rs), rs)]
        w = wu if p % 2 else wv
        return w.at[p // 2, pl.ds(pl.multiple_of((s * 2 + cc) * rs, rs), rs)]

    def local_copy(p):
        if p is final:
            src = u_ref.at[layers - 1, :, pl.ds(cols - bw, bw)]
        elif isinstance(p, tuple):
            src = u_ref.at[layers - 1, :, pl.ds(pl.multiple_of(p[0] * bw, bw), bw)]
        else:
            src = (v_ref if p % 2 == 0 else u_ref).at[p // 2]
        return pltpu.make_async_copy(src, blk(p, z, c), loc.at[0 if p == 0 else 1])

    def direct(p, k):
        return copy_to(blk(p, z, c), blk(p, z, c), zsend.at[factor(p)],
                       zrecv.at[at_sem(p), z + min(HOPS[k], 0)], dev(z + HOPS[k], c, me))

    def slot(s):
        return jnp.where(s > z, s - 1, s)

    def arrival(p, s):
        return copy_to(blk(p, s, c), blk(p, s, c), fsend.at[factor(p)],
                       zrecv.at[at_sem(p), slot(s)], dev(z, 1 - c, me))

    def relays(s):
        return ((s > z) & (z >= 1)) | ((s < z) & (z <= nz - 2))

    def relay(p, s):
        return copy_to(blk(p, s, c), blk(p, s, c), fsend.at[factor(p)], zrecv.at[at_sem(p), slot(s)],
                       dev(jnp.where(s > z, z - 1, z + 1), c, me))

    def landed(p, s):
        if isinstance(p, tuple):
            return urecv.at[layers - 1 + (nb - 1 if p is final else p[0])]
        return urecv.at[p // 2] if p % 2 else vrecv.at[p // 2, s]

    def push(p, s):
        return copy_to(blk(p, s, c), blk(p, s, c), psend.at[factor(p)], landed(p, s), dev(z, 1 - c, me))

    def halves(p, count):
        if p is final:
            return last_ref.at[pl.ds(0, count * rs)]
        if isinstance(p, tuple):
            return wu.at[layers - 1, pl.ds(0, count * rs),
                         pl.ds(pl.multiple_of(p[0] * bw, bw), bw)]
        if native and p % 2 == 0:
            return wv.at[p // 2, pl.ds(0, count), :, pl.ds(0, rs)]
        return (wu if p % 2 else wv).at[p // 2, pl.ds(0, count * rs)]

    def pushed(p, s=None):
        ref = halves(p, nz) if s is None else blk(p, s, 1 - c)
        return copy_to(ref, ref, psend.at[factor(p)], landed(p, s), dev(z, 1 - c, me))

    def sent(sem, p, count):
        ref = halves(p, count)
        copy_to(ref, ref, sem.at[p], vrecv.at[0, 0], dev(z, 1 - c, me)).wait_send()

    def held(d):
        return (z >= 1) & (z <= nz - 2)

    def to_end(k):
        return (z + HOPS[k] == 0) | (z + HOPS[k] == nz - 1)

    def issue_own(p, first, k_ok=lambda k: True):
        for k in range(len(HOPS)):
            hold = held(HOPS[k])

            @pl.when(valid(HOPS[k]) & (jnp.logical_not(hold) if first else hold) & (k_ok(k)))
            def _():
                direct(p, k).start()

    def take(p, s):
        @pl.when(s != z)
        def _():
            arrival(p, s).wait_recv()

        @pl.when(relays(s))
        def _():
            relay(p, s).start()

        push(p, s).start()

    def lanes(s):
        return pl.ds(pl.multiple_of(s * ck, ck), ck)

    def seg_rows(m):
        return pl.ds(pl.multiple_of(m * seg, seg), seg)

    def half(m, h):
        return pl.ds(pl.multiple_of(m * seg + h * (seg // 2), seg // 2), seg // 2)

    two = n == 4
    peers = (me + 1 - 2 * (me % 2), lax.rem(me + 2, n), n - 1 - me, me)

    def other(k):
        return lax.rem(me + k, n)

    whole_in = pltpu.make_async_copy(x_ref, f_ref, in_s)
    barrier = pltpu.get_barrier_semaphore()
    for m in peers[:2] if two else [other(k) for k in range(1, n)]:
        pl.semaphore_signal(barrier, inc=1, device_id=dev(z, c, m), device_id_type=MESH)
    pl.semaphore_signal(barrier, inc=1, device_id=dev(z, 1 - c, me), device_id_type=MESH)
    for d in HOPS:
        @pl.when(valid(d))
        def _():
            pl.semaphore_signal(barrier, inc=1, device_id=dev(z + d, c, me), device_id_type=MESH)
    local_copy(0).start()
    pl.semaphore_wait(barrier, (3 if two else n) + jnp.minimum(z, 1) + jnp.minimum(nz - 1 - z, 1))

    def first_sends(p):
        issue_own(p, True)
        if p == 0:
            issue_own(p, False)
        if p == 1:
            issue_own(p, False, to_end)

    def rest(body):
        for p in range(1, tail):
            body(p)
        each_tail(body)

    local_copy(0).wait()
    first_sends(0)
    rest(lambda p: local_copy(p).start())
    whole_in.start()
    rest(lambda p: local_copy(p).wait())
    rest(first_sends)
    whole_in.wait()

    @pl.when(jnp.logical_not(end))
    def _():
        @pl.loop(0, nz)
        def _(i):
            take(0, order(i))

    if tail > 1:
        issue_own(1, False, lambda k: jnp.logical_not(to_end(k)))
    if layers > 1:
        issue_own(2, False)
    else:
        each_tail(lambda p: issue_own(p, False))

    kept_ref[...] = f_ref[:, pl.ds(cols - bw, bw)]

    def early(p):
        return {0: 0, 2: min(2, nz)}.get(p, 1)

    for l in range(layers):
        pv, pu = 2 * l, 2 * l + 1
        cur = f_ref if l == 0 else out_ref
        last = l == layers - 1
        rk = rank_ref if last else rank.at[l]

        def sum_out(s, k):
            t = other(k)
            return copy_to(sbuf.at[seg_rows(t), lanes(s)], rbuf.at[l, me, :, lanes(s)],
                           rs_s, rs_r.at[s], dev(z, c, t))

        def sums_in(s):
            ref = rbuf.at[l, pl.ds(0, n - 1), :, lanes(s)]
            return copy_to(ref, ref, rs_s, rs_r.at[s], dev(z, 1 - c, me))

        def rank_out(s, k):
            mine = rk.at[seg_rows(me), lanes(s)]
            return copy_to(mine, mine, ag_s, all_r, dev(z, c, other(k)))

        def reduce(s):
            acc = pf[seg_rows(me), lanes(s)]
            sums_in(s).wait_recv()
            for k in range(1, n):
                acc = acc + rbuf[l, other(k), :, lanes(s)].astype(jnp.float32)
            rk[seg_rows(me), lanes(s)] = acc.astype(jnp.bfloat16)
            for k in range(1, n):
                rank_out(s, k).start()

        def mp_refs(kind, s):
            at, here = lanes(s), rbuf.at[l, min(kind, 5), :, lanes(s)]
            if kind < 4:
                rows_at = half(peers[(2, 2, 0, 1)[kind]], (0, 1, 0, 1)[kind])
                return sbuf.at[rows_at, at], here, rs_s, (rs_r if kind < 2 else cb_r).at[s]
            if kind < 6:
                return cbuf.at[kind - 4, :, at], here, cb_s, cb_r.at[s]
            mine = (seg_rows(me), seg_rows(me), half(peers[0], 0), half(peers[1], 1))[kind - 6]
            ref = rk.at[mine, at]
            return ref, ref, ag_s, ag_r.at[s] if kind < 8 else all_r

        def mp_out(kind, s):
            src, dst, send, recv = mp_refs(kind, s)
            return copy_to(src, dst, send, recv, dev(z, c, peers[TO_Y[kind]]))

        def got(ref, sem):
            copy_to(ref, ref, rs_s, sem, dev(z, 1 - c, me)).wait_recv()

        def gone(ref, sem):
            copy_to(ref, ref, sem, all_r, dev(z, 1 - c, me)).wait_send()

        def sum_on(s):
            at = lanes(s)
            got(rbuf.at[l, pl.ds(0, 2), :, at], rs_r.at[s])
            for h in range(2):
                cbuf[h, :, at] = (pf[half(peers[1 - h], h), at]
                                  + rbuf[l, h, :, at].astype(jnp.float32)).astype(jnp.bfloat16)
                mp_out(4 + h, s).start()

        def sum_up(s):
            at = lanes(s)
            got(rbuf.at[l, pl.ds(2, 4), :, at], cb_r.at[s])
            for h in range(2):
                acc = pf[half(me, h), at] + rbuf[l, 2 + h, :, at].astype(jnp.float32)
                acc = acc + rbuf[l, 4 + h, :, at].astype(jnp.float32)
                rk[half(me, h), at] = acc.astype(jnp.bfloat16)
            for kind in (6, 7):
                mp_out(kind, s).start()

        def pass_on(s):
            got(rk.at[pl.ds(0, 2 * seg), lanes(s)], ag_r.at[s])
            for kind in (8, 9):
                mp_out(kind, s).start()

        def exchange(i, stages):
            for lag, stage in stages:
                @pl.when((i >= lag) & (i < nz + lag))
                def _():
                    stage(order(i - lag))

        steps = ((1, sum_on), (2, sum_up), (3, pass_on)) if two else ((1, reduce),)

        each_up = each_tail if last else lambda body: body(pu)

        @pl.loop(0, nz)
        def _(i):
            s = order(i)

            if two:
                exchange(i, steps)
            else:
                @pl.when(i == nz - 1)
                def _():
                    reduce(order(i - 1))

            @pl.when(end & (i >= early(pv)))
            def _():
                take(pv, s)

            @pl.when(jnp.logical_not(end))
            def _():
                each_up(lambda p: take(p, s))

            pushed(pv, s).wait_recv()
            if native:
                part = jnp.dot(cur[...], wv[l, s], preferred_element_type=jnp.float32)
            else:
                part = lax.dot_general(cur[...], wv[l, lanes(s), :], (((1,), (1,)), ((), ())),
                                       preferred_element_type=jnp.float32)
            pf[:, lanes(s)] = part
            sbuf[:, lanes(s)] = part.astype(jnp.bfloat16)
            if two:
                for kind in range(4):
                    mp_out(kind, s).start()
            else:
                for k in range(1, n):
                    sum_out(s, k).start()

                @pl.when((i > 0) & (i < nz - 1))
                def _():
                    reduce(order(i - 1))

        if pu + 2 < tail:
            issue_own(pu + 2, False)
        elif not last and layers > 2:
            issue_own(pv + 2, False)

        if two:
            @pl.loop(nz, nz + 3)
            def _(i):
                exchange(i, steps)
        else:
            reduce(order(nz - 1))

        @pl.loop(0, nz - 1)
        def _(i):
            s = order(i)

            @pl.when(end)
            def _():
                each_up(lambda p: take(p, s))

            if not last:
                @pl.when(jnp.logical_not(end))
                def _():
                    take(pv + 2, s)

        if not last:
            @pl.when(jnp.logical_not(end))
            def _():
                take(pv + 2, order(nz - 1))

            if pv + 4 < tail - 1:
                issue_own(pv + 4, False)
            elif pv + 4 > tail:
                each_tail(lambda p: issue_own(p, False))

        if last:
            @pl.when(end)
            def _():
                for p in range(tail):
                    sent(zsend, p, 1)
                    sent(psend, p, nz)
                sent(zsend, tail, 1)

        if not last:
            @pl.when(end)
            def _():
                for i in range(early(pv + 2)):
                    take(pv + 2, order(i))

        if two:
            got(rk.at[pl.ds(0, seg)], all_r)
            gone(sbuf.at[pl.ds(0, 2 * seg)], rs_s)
            gone(cbuf, cb_s)
            gone(rk.at[pl.ds(0, 3 * seg)], ag_s)
        else:
            got(rk.at[pl.ds(0, (n - 1) * seg)], all_r)
            gone(sbuf.at[pl.ds(0, (n - 1) * seg)], rs_s)
            gone(rk.at[pl.ds(0, (n - 1) * seg)], ag_s)

        if last:
            @pl.when(end)
            def _():
                take((0,) if nb > 1 else final, order(nz - 1))

        def finish(p):
            @pl.when(end)
            def _():
                if last:
                    if p is not final:
                        @pl.when(p[0] < nb - 2)
                        def _():
                            take((p[0] + 1,), order(nz - 1))

                        @pl.when(p[0] == nb - 2)
                        def _():
                            take(final, order(nz - 1))
                else:
                    take(p, order(nz - 1))

            pushed(p).wait_recv()
            if p is final:
                return
            width, base = (bw, p[0] * bw) if last else (cols, 0)

            @pl.loop(0, width // cb)
            def _(j):
                at = pl.ds(pl.multiple_of(base + j * cb, cb), cb)
                cross = jnp.dot(rk[...], wu[l, :, at], preferred_element_type=jnp.float32)
                cross = cross + b_ref[l, at][None, :]
                out_ref[:, at] = (f_ref[:, at].astype(jnp.float32) * cross
                                  + cur[:, at].astype(jnp.float32)).astype(jnp.bfloat16)

        each_up(finish)

    sent(psend, tail, nz)

    @pl.when(jnp.logical_not(end))
    def _():
        for p in range(tail + 1):
            sent(zsend, p, 2)
            sent(fsend, p, nz - 1)
            if p < tail:
                sent(psend, p, nz)


def last_block(x_ref, rank_ref, u_ref, b_ref, f_ref, y_ref, block, sems):
    cols, bw = x_ref.shape[1], u_ref.shape[1]
    done, at = pl.ds(0, cols - bw), pl.ds(cols - bw, bw)
    store = pltpu.make_async_copy(block, y_ref.at[:, at], sems.at[0])
    if cols > bw:
        ready = pltpu.make_async_copy(x_ref.at[:, done], y_ref.at[:, done], sems.at[1])
        ready.start()
    cross = jnp.dot(rank_ref[...], u_ref[...], preferred_element_type=jnp.float32)
    cross = cross + b_ref[b_ref.shape[0] - 1, at][None, :]
    block[...] = (f_ref[...].astype(jnp.float32) * cross
                  + x_ref[:, at].astype(jnp.float32)).astype(jnp.bfloat16)
    store.start()
    if cols > bw:
        ready.wait()
    store.wait()


def solution(mesh):
    n = mesh.shape["mp"]
    nz = mesh.shape["dp"] // 2

    def local(features, v_weight, u_weight, cross_bias):
        layers, rs, cols = u_weight.shape
        rows = features.shape[0]
        r = rs * nz * 2
        nb = cols // 256 if cols % 256 == 0 else 1
        pieces = 2 * layers - 1 + nb
        native = rs % 128 == 0
        v = v_weight if native else jnp.swapaxes(v_weight, 1, 2)
        vm = pl.BlockSpec(memory_space=pltpu.VMEM)
        hbm = pl.BlockSpec(memory_space=pl.ANY)
        dma = pltpu.SemaphoreType.DMA
        crossed, rank, u_last, kept = pl.pallas_call(
            functools.partial(kernel, nz, n, native, nb),
            out_shape=(pltpu.VMEM((rows, cols), jnp.bfloat16), pltpu.VMEM((rows, r), jnp.bfloat16),
                       pltpu.VMEM((r, cols // nb), jnp.bfloat16),
                       pltpu.VMEM((rows, cols // nb), jnp.bfloat16)),
            in_specs=[hbm, hbm, hbm, vm],
            out_specs=(vm, vm, vm, vm),
            scratch_shapes=[
                pltpu.VMEM((layers, nz, cols, 2 * rs) if native else (layers, r, cols), jnp.bfloat16),
                pltpu.VMEM((layers, r, cols), jnp.bfloat16),
                pltpu.VMEM((rows, cols), jnp.bfloat16),
                pltpu.VMEM((rows, r), jnp.float32),
                pltpu.VMEM((rows, r), jnp.bfloat16),
                pltpu.VMEM((layers, 6, rows // (2 * n), r) if n == 4 else (layers, n, rows // n, r),
                           jnp.bfloat16),
                pltpu.VMEM((max(layers - 1, 1), rows, r), jnp.bfloat16),
                dma((2,)), dma((2 * layers,)), dma((pieces, nz - 1)), dma((2 * layers,)), dma((2 * layers,)),
                dma((layers, nz)), dma((layers - 1 + nb,)),
                pltpu.VMEM((2, rows // (2 * n), r), jnp.bfloat16),
                dma, dma, dma, dma((nz,)), dma((nz,)), dma((nz,)), dma, dma,
            ],
            compiler_params=pltpu.CompilerParams(
                collective_id=0, has_side_effects=True, vmem_limit_bytes=55 * 2**20),
            name="cross_layers",
        )(v, u_weight, features, cross_bias)
        return pl.pallas_call(
            last_block,
            out_shape=jax.ShapeDtypeStruct((rows, cols), jnp.bfloat16),
            in_specs=[vm, vm, vm, vm, vm],
            out_specs=hbm,
            scratch_shapes=[pltpu.VMEM((rows, cols // nb), jnp.bfloat16), dma((2,))],
            compiler_params=pltpu.CompilerParams(vmem_limit_bytes=16 * 2**20),
            name="last_block",
        )(crossed, rank, u_last, cross_bias, kept)

    return jax.shard_map(
        local,
        mesh=mesh,
        in_specs=(P("dp", "mp"), P(None, "mp", "dp"), P(None, "dp", "mp"), P(None, "mp")),
        out_specs=P("dp", "mp"),
        check_vma=False,
    )
```
